32 devices in a mesh: dp: 4 (over y, x), ctx: 4 (over z), tensor: 2 (over core).
Axes of the slice: x: 2, y: 2, z: 4, core: 2. Of those that a mesh axis runs over, the one named last changes fastest.
Arguments:
- block_input: bfloat16 [4, 2048, 1536], P('dp', 'ctx'), may hold values from -6 to 6
- segments: int32 [4, 2048], P('dp'), may hold values from 0 to 31, as said below
- positions: int32 [4, 2048], P('dp', 'ctx'), may hold values from 0 to 1023, as said below
- cotangent: bfloat16 [4, 2048, 1536], P('dp', 'ctx'), may hold values from -6 to 6
- norm1_gain: float32 [1536], replicated, may hold values from 0.1 to 1.9
- w_query: bfloat16 [1536, 1536], P(None, 'tensor'), may hold values from -0.15625 to 0.15625
- w_key: bfloat16 [1536, 768], P(None, 'tensor'), may hold values from -0.15625 to 0.15625
- w_value: bfloat16 [1536, 768], P(None, 'tensor'), may hold values from -0.15625 to 0.15625
- w_out: bfloat16 [1536, 1536], P('tensor'), may hold values from -0.625 to 0.625
- norm2_gain: float32 [1536], replicated, may hold values from 0.1 to 1.9
- w_gate: bfloat16 [1536, 4096], P(None, 'tensor'), may hold values from -0.15625 to 0.15625
- w_up: bfloat16 [1536, 4096], P(None, 'tensor'), may hold values from -0.15625 to 0.15625
- w_down: bfloat16 [4096, 1536], P('tensor'), may hold values from -0.09375 to 0.09375
Outputs:
- block_output: bfloat16 [4, 2048, 1536], P('dp', 'ctx')
- grad_input: bfloat16 [4, 2048, 1536], P('dp', 'ctx')
- grad_norm1: float32 [1536], replicated
- grad_query: float32 [1536, 1536], P(None, 'tensor')
- grad_key: float32 [1536, 768], P(None, 'tensor')
- grad_value: float32 [1536, 768], P(None, 'tensor')
- grad_out: float32 [1536, 1536], P('tensor')
- grad_norm2: float32 [1536], replicated
- grad_gate: float32 [1536, 4096], P(None, 'tensor')
- grad_up: float32 [1536, 4096], P(None, 'tensor')
- grad_down: float32 [4096, 1536], P('tensor')
The draws below stay inside these ranges and needn't reach their ends.
Inputs may be any that keep to these rules, and one draw needn't show every extreme that they name: `segments`: along each sequence the document numbers start at 0, never fall, rise by at most one at a time and only at multiples of 64 positions; every document spans at most 1024 positions. `positions`: each token's position counted from the start of its document.
All inputs are finite; a program needn't handle non-finite values.
Results may differ from the reference program's by a relative error of at most 0.025.
Values may be sent and summed in bfloat16 or wider, within the bound.
A program may use at most 320 MiB of HBM per device.

```python
import jax
import jax.numpy as jnp
from jax import lax

D = 1536
H = 16
KVH = 8
HDIM = 96
FF = 4096
LEN = 2048
SEQS = 4
N_TENSOR = 2


def document_layout(key):
    block_count = 32
    block_size = LEN // 32
    flip_key = jax.random.fold_in(key, 11)
    phase_key = jax.random.fold_in(key, 12)
    start_key = jax.random.fold_in(key, 13)
    single_key = jax.random.fold_in(key, 14)
    block_ids = jnp.arange(block_count, dtype=jnp.int32)[None, :]
    seq_ids = jnp.arange(SEQS, dtype=jnp.int32)[:, None]
    random_flips = (jax.random.randint(flip_key, (SEQS, block_count), 0, 4) == 0).astype(jnp.int32)
    phase = jax.random.randint(phase_key, (SEQS, 1), 0, 16).astype(jnp.int32)
    forced = (block_ids - phase) % 16 == 0
    flips = jnp.where(forced, 1, random_flips).astype(jnp.int32)
    long_start = jax.random.randint(start_key, (), 1, 8).astype(jnp.int32)
    inside_long = (block_ids > long_start) & (block_ids < long_start + 16)
    first_flips = jnp.where(inside_long, 0, 1).astype(jnp.int32)
    flips = jnp.where(seq_ids == 0, first_flips, flips)
    single_seq = jax.random.randint(single_key, (), 1, SEQS).astype(jnp.int32)
    flips = jnp.where(seq_ids == single_seq, 1, flips)
    flips = jnp.where(block_ids == 0, 0, flips).astype(jnp.int32)
    seg_blocks = jnp.cumsum(flips, axis=1).astype(jnp.int32)
    start_blocks = lax.cummax(jnp.where(flips == 1, block_ids, 0).astype(jnp.int32), axis=1)
    seg_tokens = jnp.repeat(seg_blocks, block_size, axis=1).astype(jnp.int32)
    pos_tokens = jnp.arange(LEN, dtype=jnp.int32)[None, :] - jnp.repeat(start_blocks, block_size, axis=1) * block_size
    return (seg_tokens, pos_tokens.astype(jnp.int32))


def draw_segments(key, part):
    return document_layout(key)[0]


def draw_positions(key, part):
    return document_layout(key)[1]


def steps_of(key, extent, split, least, top_value):
    factor_of, own = 1.0, jax.random.fold_in(key, 6)
    for position, shards_of in split:
        heights = jnp.exp(jax.random.uniform(jax.random.fold_in(own, position), (shards_of,), jnp.float32, least / len(split), top_value / len(split)))
        factor_of = factor_of * jnp.repeat(heights, extent[position] // shards_of).reshape([-1 if axis == position else 1 for axis in range(len(extent))])
    return factor_of


def centred(stream_key, extent, scale, reach, cuts=(), held_as=jnp.bfloat16):
    result = jax.random.normal(stream_key, extent, jnp.float32) * scale
    if len(cuts) > 0:
        result = steps_of(stream_key, extent, cuts, -0.22, 0.18) * result
    return jnp.clip(result, min=-reach, max=reach).astype(held_as)


def setup_inputs(seed: int = 0) -> dict:
    seeds = jax.random.split(jax.random.key(seed), 14)
    block_input = centred(seeds[0], (SEQS, LEN, D), 1.0, 6.0, ((0, 4), (1, 4)))
    segments = draw_segments(jax.random.fold_in(seeds[13], 71), 0)
    positions = draw_positions(jax.random.fold_in(seeds[13], 71), 0)
    cotangent = centred(seeds[3], (SEQS, LEN, D), 1.0, 6.0, ((0, 4), (1, 4)))
    norm1_gain = jnp.clip(1.0 + 0.18 * jax.random.normal(seeds[4], (D,), jnp.float32), 0.1, 1.9)
    w_query = centred(seeds[5], (D, H * HDIM), D ** -0.5, 0.15625, ((1, 2),))
    w_key = centred(seeds[6], (D, KVH * HDIM), D ** -0.5, 0.15625, ((1, 2),))
    w_value = centred(seeds[7], (D, KVH * HDIM), D ** -0.5, 0.15625, ((1, 2),))
    w_out = centred(seeds[8], (H * HDIM, D), (H * HDIM // 16) ** -0.5, 0.625, ((0, 2),))
    norm2_gain = jnp.clip(1.0 + 0.18 * jax.random.normal(seeds[9], (D,), jnp.float32), 0.1, 1.9)
    w_gate = centred(seeds[10], (D, FF), D ** -0.5, 0.15625, ((1, 2),))
    w_up = centred(seeds[11], (D, FF), D ** -0.5, 0.15625, ((1, 2),))
    w_down = centred(seeds[12], (FF, D), FF ** -0.5, 0.09375, ((0, 2),))
    return dict(block_input=block_input, segments=segments, positions=positions, cotangent=cotangent, norm1_gain=norm1_gain, w_query=w_query, w_key=w_key, w_value=w_value, w_out=w_out, norm2_gain=norm2_gain, w_gate=w_gate, w_up=w_up, w_down=w_down)


EPSILON = 1e-05
THETA_BASE = 100000.0
MASKED_SCORE = -1e+30

def rotate(tensor_in, where, sign):
    half = tensor_in.shape[-1] // 2
    freqs = THETA_BASE ** (-(jnp.arange(half, dtype=jnp.float32) * 2.0) / tensor_in.shape[-1])
    angles = where.astype(jnp.float32)[..., None] * freqs
    cosine = jnp.cos(angles)[..., None, :]
    sine = sign * jnp.sin(angles)[..., None, :]
    first = tensor_in[..., :half]
    second = tensor_in[..., half:]
    return jnp.concatenate([first * cosine - second * sine, second * cosine + first * sine], axis=-1)

def shard_sum(pairs):
    total = None
    for left, right in pairs:
        left_parts = left.reshape(left.shape[0], N_TENSOR, -1).astype(jnp.float32)
        right_parts = right.reshape(N_TENSOR, -1, right.shape[1]).astype(jnp.float32)
        partial_sum = jnp.einsum('ltc,tcd->ltd', left_parts, right_parts, precision=lax.Precision.HIGHEST)
        total = partial_sum if total is None else total + partial_sum
    rounded = lax.optimization_barrier(total.astype(jnp.bfloat16))
    return lax.optimization_barrier(jnp.sum(rounded.astype(jnp.float32), axis=1))

def tdot(left, right):
    return lax.dot_general(left, right, (((0,), (0,)), ((), ())), preferred_element_type=jnp.float32)

def rdot(left, right):
    return lax.dot_general(left, right, (((1,), (1,)), ((), ())), preferred_element_type=jnp.float32)

def masked_scores(query_rows, key_all, seg_query, seg_keys, query_index, scale):
    length = key_all.shape[0]
    raw_scores = jnp.einsum('qkgd,skd->kgqs', query_rows.astype(jnp.float32), key_all.astype(jnp.float32), precision=lax.Precision.HIGHEST) * scale
    allowed = (seg_query[:, None] == seg_keys[None, :]) & (jnp.arange(length, dtype=jnp.int32)[None, :] <= query_index[:, None])
    return jnp.where(allowed, raw_scores, MASKED_SCORE)

def reference(block_input, segments, positions, cotangent, norm1_gain, w_query, w_key, w_value, w_out, norm2_gain, w_gate, w_up, w_down):
    scale = HDIM ** (-0.5)
    group = H // KVH
    qblock = min(512, LEN)
    nblocks = LEN // qblock

    def one_sequence(totals, items):
        x_seq, seg_row, pos_row, dy_seq = items
        inputs = x_seq.astype(jnp.float32)
        inv_one = lax.rsqrt(lax.optimization_barrier(jnp.mean(inputs * inputs, axis=1, keepdims=True)) + EPSILON)
        normed1 = (inputs * inv_one * norm1_gain).astype(jnp.bfloat16)
        queries = rotate(jnp.dot(normed1, w_query, preferred_element_type=jnp.float32).reshape(LEN, H, HDIM), pos_row, 1.0).astype(jnp.bfloat16)
        keys = rotate(jnp.dot(normed1, w_key, preferred_element_type=jnp.float32).reshape(LEN, KVH, HDIM), pos_row, 1.0).astype(jnp.bfloat16)
        values = jnp.dot(normed1, w_value, preferred_element_type=jnp.float32).astype(jnp.bfloat16).reshape(LEN, KVH, HDIM)

        def forward_block(block_id):
            start = block_id * qblock
            query_rows = lax.dynamic_slice_in_dim(queries, start, qblock, 0).reshape(qblock, KVH, group, HDIM)
            seg_query = lax.dynamic_slice_in_dim(seg_row, start, qblock, 0)
            query_index = start + jnp.arange(qblock, dtype=jnp.int32)
            scores = masked_scores(query_rows, keys, seg_query, seg_row, query_index, scale)
            row_max = lax.optimization_barrier(jnp.max(scores, axis=-1))
            log_total = row_max + jnp.log(lax.optimization_barrier(jnp.sum(jnp.exp(scores - row_max[..., None]), axis=-1)))
            probs = jnp.exp(scores - log_total[..., None]).astype(jnp.bfloat16)
            block_out = jnp.einsum('kgqs,skd->qkgd', probs.astype(jnp.float32), values.astype(jnp.float32), precision=lax.Precision.HIGHEST)
            return (block_out.reshape(qblock, H * HDIM).astype(jnp.bfloat16), log_total)
        outs_blocks, log_totals = lax.map(forward_block, jnp.arange(nblocks, dtype=jnp.int32))
        attended = outs_blocks.reshape(LEN, H * HDIM)
        attn_branch = shard_sum([(attended, w_out)])
        hidden = inputs + attn_branch
        inv_two = lax.rsqrt(lax.optimization_barrier(jnp.mean(hidden * hidden, axis=1, keepdims=True)) + EPSILON)
        normed2 = (hidden * inv_two * norm2_gain).astype(jnp.bfloat16)
        gate = jnp.dot(normed2, w_gate, preferred_element_type=jnp.float32)
        upper = jnp.dot(normed2, w_up, preferred_element_type=jnp.float32)
        sigmoid_gate = jax.nn.sigmoid(gate)
        activated = gate * sigmoid_gate
        mixed = (activated * upper).astype(jnp.bfloat16)
        ffn_branch = shard_sum([(mixed, w_down)])
        block_out = (hidden + ffn_branch).astype(jnp.bfloat16)
        grad_down = tdot(mixed, dy_seq)
        grad_mixed = rdot(dy_seq, w_down)
        grad_gate_act = (grad_mixed * upper * sigmoid_gate * (1.0 + gate * (1.0 - sigmoid_gate))).astype(jnp.bfloat16)
        grad_upper = (grad_mixed * activated).astype(jnp.bfloat16)
        grad_wgate = tdot(normed2, grad_gate_act)
        grad_wup = tdot(normed2, grad_upper)
        grad_normed2 = shard_sum([(grad_gate_act, w_gate.T), (grad_upper, w_up.T)])
        scaled_two = grad_normed2 * norm2_gain
        grad_gain_two = lax.optimization_barrier(jnp.sum(grad_normed2 * hidden * inv_two, axis=0))
        grad_hidden = dy_seq.astype(jnp.float32) + inv_two * scaled_two - hidden * (inv_two * inv_two * inv_two) * lax.optimization_barrier(jnp.mean(scaled_two * hidden, axis=1, keepdims=True))
        grad_branch = grad_hidden.astype(jnp.bfloat16)
        grad_wout = tdot(attended, grad_branch)
        grad_attended = rdot(grad_branch, w_out).astype(jnp.bfloat16)

        def backward_block(carry, block_id):
            start = block_id * qblock
            query_rows = lax.dynamic_slice_in_dim(queries, start, qblock, 0).reshape(qblock, KVH, group, HDIM)
            out_rows = lax.dynamic_slice_in_dim(attended, start, qblock, 0).reshape(qblock, KVH, group, HDIM)
            grad_rows = lax.dynamic_slice_in_dim(grad_attended, start, qblock, 0).reshape(qblock, KVH, group, HDIM)
            seg_query = lax.dynamic_slice_in_dim(seg_row, start, qblock, 0)
            query_index = start + jnp.arange(qblock, dtype=jnp.int32)
            scores = masked_scores(query_rows, keys, seg_query, seg_row, query_index, scale)
            log_total = lax.dynamic_index_in_dim(log_totals, block_id, 0, keepdims=False)
            probs = jnp.exp(scores - log_total[..., None])
            probs_half = probs.astype(jnp.bfloat16).astype(jnp.float32)
            delta = lax.optimization_barrier(jnp.sum(grad_rows.astype(jnp.float32) * out_rows.astype(jnp.float32), axis=3)).transpose(1, 2, 0)
            grad_probs = jnp.einsum('qkgd,skd->kgqs', grad_rows.astype(jnp.float32), values.astype(jnp.float32), precision=lax.Precision.HIGHEST)
            grad_scores = (probs * (grad_probs - delta[..., None])).astype(jnp.bfloat16).astype(jnp.float32)
            grad_q = jnp.einsum('kgqs,skd->qkgd', grad_scores, keys.astype(jnp.float32), precision=lax.Precision.HIGHEST) * scale
            grad_k = jnp.einsum('kgqs,qkgd->skd', grad_scores, query_rows.astype(jnp.float32), precision=lax.Precision.HIGHEST) * scale
            grad_v = jnp.einsum('kgqs,qkgd->skd', probs_half, grad_rows.astype(jnp.float32), precision=lax.Precision.HIGHEST)
            return ((carry[0] + grad_k, carry[1] + grad_v), grad_q.reshape(qblock, H, HDIM))
        zero_kv = jnp.zeros((LEN, KVH, HDIM), jnp.float32)
        (grad_keys_raw, grad_values_raw), grad_q_blocks = lax.scan(backward_block, (zero_kv, zero_kv), jnp.arange(nblocks, dtype=jnp.int32))
        grad_queries = rotate(grad_q_blocks.reshape(LEN, H, HDIM), pos_row, -1.0).astype(jnp.bfloat16).reshape(LEN, H * HDIM)
        grad_keys = rotate(grad_keys_raw, pos_row, -1.0).astype(jnp.bfloat16).reshape(LEN, KVH * HDIM)
        grad_values = grad_values_raw.astype(jnp.bfloat16).reshape(LEN, KVH * HDIM)
        grad_wquery = tdot(normed1, grad_queries)
        grad_wkey = tdot(normed1, grad_keys)
        grad_wvalue = tdot(normed1, grad_values)
        grad_normed1 = shard_sum([(grad_queries, w_query.T), (grad_keys, w_key.T), (grad_values, w_value.T)])
        scaled_one = grad_normed1 * norm1_gain
        grad_gain_one = lax.optimization_barrier(jnp.sum(grad_normed1 * inputs * inv_one, axis=0))
        grad_in = (grad_hidden + inv_one * scaled_one - inputs * (inv_one * inv_one * inv_one) * lax.optimization_barrier(jnp.mean(scaled_one * inputs, axis=1, keepdims=True))).astype(jnp.bfloat16)
        new_totals = (totals[0] + grad_gain_one, totals[1] + grad_wquery, totals[2] + grad_wkey, totals[3] + grad_wvalue, totals[4] + grad_wout, totals[5] + grad_gain_two, totals[6] + grad_wgate, totals[7] + grad_wup, totals[8] + grad_down)
        return (new_totals, (block_out, grad_in))
    zeros_init = (jnp.zeros((D,), jnp.float32), jnp.zeros((D, H * HDIM), jnp.float32), jnp.zeros((D, KVH * HDIM), jnp.float32), jnp.zeros((D, KVH * HDIM), jnp.float32), jnp.zeros((H * HDIM, D), jnp.float32), jnp.zeros((D,), jnp.float32), jnp.zeros((D, FF), jnp.float32), jnp.zeros((D, FF), jnp.float32), jnp.zeros((FF, D), jnp.float32))
    totals, (outputs, grads_in) = lax.scan(one_sequence, zeros_init, (block_input, segments, positions, cotangent))
    return (outputs, grads_in, totals[0], totals[1], totals[2], totals[3], totals[4], totals[5], totals[6], totals[7], totals[8])
```

```python
import jax
import jax.numpy as jnp
from jax import lax
from jax.sharding import PartitionSpec as P

HDIM = 96
MAX_SPAN = 1024

EPSILON = 1e-05
THETA_BASE = 100000.0
MASKED_SCORE = -1e30


F32 = jnp.float32
BF16 = jnp.bfloat16

FLIP_X = [(0, 1), (1, 0), (2, 3), (3, 2)]
FLIP_Y = [(0, 2), (2, 0), (1, 3), (3, 1)]
INWARD = [(0, 1), (3, 2)]
MIDDLE = [(1, 2), (2, 1)]
OUTWARD = [(1, 0), (2, 3)]


def rotate(tensor_in, where, sign):
    half = tensor_in.shape[-1] // 2
    freqs = THETA_BASE ** (-(jnp.arange(half, dtype=F32) * 2.0) / tensor_in.shape[-1])
    angles = where.astype(F32)[..., None] * freqs
    cosine = jnp.cos(angles)[..., None, :]
    sine = sign * jnp.sin(angles)[..., None, :]
    first = tensor_in[..., :half]
    second = tensor_in[..., half:]
    return jnp.concatenate(
        [first * cosine - second * sine, second * cosine + first * sine], axis=-1
    )


def dot(left, right):
    return jnp.dot(left, right, preferred_element_type=F32)


def tdot(left, right):
    return lax.dot_general(left, right, (((0,), (0,)), ((), ())), preferred_element_type=F32)


def rdot(left, right):
    return lax.dot_general(left, right, (((1,), (1,)), ((), ())), preferred_element_type=F32)


def tensor_sum(share, n_tensor):
    if n_tensor == 2:
        other = lax.ppermute(share, "tensor", [(0, 1), (1, 0)])
        return share.astype(F32) + other.astype(F32)
    return lax.psum(share, "tensor").astype(F32)


class Axis:
    def __init__(self, name, pairs, bit):
        self.name = name
        self.pairs = pairs
        self.bit = bit

    def swap(self, value):
        return lax.ppermute(value, self.name, self.pairs)

    def scatter(self, value):
        half = value.shape[0] // 2
        keep = lax.dynamic_slice_in_dim(value, self.bit * half, half, 0)
        send = lax.dynamic_slice_in_dim(value, (1 - self.bit) * half, half, 0)
        return add(keep, self.swap(send))

    def gather(self, value, dtype=BF16):
        other = self.swap(value)
        low = jnp.where(self.bit == 0, value, other)
        high = jnp.where(self.bit == 0, other, value)
        return jnp.concatenate([low, high], axis=0).astype(dtype)


def add(left, right):
    return (left.astype(F32) + right.astype(F32)).astype(BF16)


def line_sum(value, place):
    value = add(value, lax.ppermute(value, "ctx", INWARD))
    value = add(value, lax.ppermute(value, "ctx", MIDDLE))
    outer = lax.ppermute(value, "ctx", OUTWARD)
    return jnp.where((place == 1) | (place == 2), value, outer)


def reduce_chunk(value, kind, axes, place):
    x_axis, y_axis, z_axis, w_axis = axes
    order = {
        "A1": (x_axis, y_axis),
        "A2": (y_axis, x_axis),
        "B1": (z_axis, x_axis, y_axis),
        "B2": (z_axis, y_axis, x_axis),
    }[kind]
    for axis in order:
        value = axis.scatter(value)
    if kind[0] == "A":
        value = line_sum(value, place)
    else:
        value = add(value, w_axis.swap(value))
    for axis in order[:0:-1]:
        value = axis.gather(value)
    return order[0].gather(value, F32)


def reduce_weight(partial, kinds, axes, place):
    rows = partial.shape[0] // len(kinds)
    pieces = [
        reduce_chunk(partial[i * rows : (i + 1) * rows], kind, axes, place)
        for i, kind in enumerate(kinds)
    ]
    return pieces[0] if len(pieces) == 1 else jnp.concatenate(pieces, axis=0)


def make_shards(n_dp, n_ctx, n_tensor):
    def shards(
        block_input,
        segments,
        positions,
        cotangent,
        norm1_gain,
        w_query,
        w_key,
        w_value,
        w_out,
        norm2_gain,
        w_gate,
        w_up,
        w_down,
    ):
        seq_count, stretch, width = block_input.shape
        assert seq_count == 1 and n_dp == 4 and n_ctx == 4
        heads_q = w_query.shape[1] // HDIM
        heads_kv = w_key.shape[1] // HDIM
        group = heads_q // heads_kv
        kv_width = w_key.shape[1]
        scale = HDIM ** (-0.5)
        before = min(n_ctx - 1, -(-(MAX_SPAN - 1) // stretch))
        length = (before + 1) * stretch
        dp_id = lax.axis_index("dp")
        place = lax.axis_index("ctx")
        axes = (
            Axis("dp", FLIP_X, dp_id % 2),
            Axis("dp", FLIP_Y, dp_id // 2),
            Axis("ctx", FLIP_X, place % 2),
            Axis("ctx", FLIP_Y, place // 2),
        )
        position = positions.reshape(stretch)
        inputs = block_input.reshape(stretch, width).astype(F32)
        inv_one = lax.rsqrt(jnp.mean(inputs * inputs, axis=1, keepdims=True) + EPSILON)
        normed1 = (inputs * inv_one * norm1_gain).astype(BF16)
        keys = rotate(dot(normed1, w_key).reshape(stretch, heads_kv, HDIM), position, 1.0)
        values = dot(normed1, w_value).astype(BF16)
        local_kv = jnp.concatenate([keys.astype(BF16).reshape(stretch, kv_width), values], axis=1)
        parts = [local_kv]
        for back in range(1, before + 1):
            pairs = [(i, i + back) for i in range(n_ctx - back)]
            parts.insert(0, lax.ppermute(local_kv, "ctx", pairs))
        queries = (
            rotate(dot(normed1, w_query).reshape(stretch, heads_q, HDIM), position, 1.0)
            .astype(BF16)
            .reshape(stretch, heads_kv, group, HDIM)
        )
        whole_kv = jnp.concatenate(parts, axis=0)
        key_all = whole_kv[:, :kv_width].reshape(length, heads_kv, HDIM)
        value_all = whole_kv[:, kv_width:].reshape(length, heads_kv, HDIM)

        seg_row = segments.reshape(-1)
        padded = jnp.concatenate([jnp.full((length - stretch,), -1, jnp.int32), seg_row])
        seg_keys = lax.dynamic_slice_in_dim(padded, place * stretch, length, 0)
        seg_query = lax.dynamic_slice_in_dim(seg_row, place * stretch, stretch, 0)
        allowed = (seg_query[:, None] == seg_keys[None, :]) & (
            jnp.arange(length, dtype=jnp.int32)[None, :]
            <= (length - stretch) + jnp.arange(stretch, dtype=jnp.int32)[:, None]
        )

        def masked():
            raw = jnp.einsum("qkgd,skd->kgqs", queries, key_all, preferred_element_type=F32)
            return jnp.where(allowed, raw * scale, MASKED_SCORE)

        scores = masked()
        row_max = jnp.max(scores, axis=-1)
        log_total = row_max + jnp.log(jnp.sum(jnp.exp(scores - row_max[..., None]), axis=-1))
        probs = jnp.exp(scores - log_total[..., None]).astype(BF16)
        attended = (
            jnp.einsum("kgqs,skd->qkgd", probs, value_all, preferred_element_type=F32)
            .reshape(stretch, heads_q * HDIM)
            .astype(BF16)
        )
        hidden = inputs + tensor_sum(dot(attended, w_out).astype(BF16), n_tensor)
        inv_two = lax.rsqrt(jnp.mean(hidden * hidden, axis=1, keepdims=True) + EPSILON)
        normed2 = (hidden * inv_two * norm2_gain).astype(BF16)
        gate = dot(normed2, w_gate)
        upper = dot(normed2, w_up)
        sigmoid_gate = jax.nn.sigmoid(gate)
        activated = gate * sigmoid_gate
        mixed = (activated * upper).astype(BF16)
        grad_rows_out = cotangent.reshape(stretch, width)
        grad_mixed = rdot(grad_rows_out, w_down)
        grad_gate_act = (
            grad_mixed * upper * sigmoid_gate * (1.0 + gate * (1.0 - sigmoid_gate))
        ).astype(BF16)
        grad_upper = (grad_mixed * activated).astype(BF16)

        grad_wdown = reduce_weight(
            tdot(mixed, grad_rows_out).astype(BF16), ("A1", "A2"), axes, place
        )
        grad_wgate = reduce_weight(
            tdot(normed2, grad_gate_act).astype(BF16), ("B1", "B2"), axes, place
        )
        grad_wup = reduce_weight(
            tdot(normed2, grad_upper).astype(BF16), ("A1", "A2"), axes, place
        )

        grad_normed2 = tensor_sum(
            (rdot(grad_gate_act, w_gate) + rdot(grad_upper, w_up)).astype(BF16), n_tensor
        )
        scaled_two = grad_normed2 * norm2_gain
        grad_gain_two = jnp.sum(grad_normed2 * hidden * inv_two, axis=0)
        grad_hidden = (
            grad_rows_out.astype(F32)
            + inv_two * scaled_two
            - hidden
            * (inv_two * inv_two * inv_two)
            * jnp.mean(scaled_two * hidden, axis=1, keepdims=True)
        )
        grad_branch = grad_hidden.astype(BF16)
        grad_wout = reduce_weight(
            tdot(attended, grad_branch).astype(BF16), ("B1", "B2"), axes, place
        )
        ffn_branch = tensor_sum(dot(mixed, w_down).astype(BF16), n_tensor)
        block_output = (hidden + ffn_branch).astype(BF16).reshape(1, stretch, width)

        grad_attended = rdot(grad_branch, w_out).astype(BF16)
        out_rows = attended.reshape(stretch, heads_kv, group, HDIM)
        grad_rows = grad_attended.reshape(stretch, heads_kv, group, HDIM)
        probs = jnp.exp(masked() - log_total[..., None])
        delta = jnp.sum(grad_rows.astype(F32) * out_rows.astype(F32), axis=3).transpose(1, 2, 0)
        grad_probs = jnp.einsum(
            "qkgd,skd->kgqs", grad_rows, value_all, preferred_element_type=F32
        )
        grad_scores = (probs * (grad_probs - delta[..., None])).astype(BF16)
        grad_k = (
            jnp.einsum("kgqs,qkgd->skd", grad_scores, queries, preferred_element_type=F32) * scale
        )
        grad_v = jnp.einsum(
            "kgqs,qkgd->skd", probs.astype(BF16), grad_rows, preferred_element_type=F32
        )
        grad_kv = jnp.concatenate(
            [grad_k.reshape(length, kv_width), grad_v.reshape(length, kv_width)], axis=1
        )
        grad_kv_local = grad_kv[length - stretch :]
        for back in range(1, before + 1):
            start = length - (back + 1) * stretch
            pairs = [(i + back, i) for i in range(n_ctx - back)]
            sent = grad_kv[start : start + stretch].astype(BF16)
            grad_kv_local = grad_kv_local + lax.ppermute(sent, "ctx", pairs).astype(F32)
        grad_q = (
            jnp.einsum("kgqs,skd->qkgd", grad_scores, key_all, preferred_element_type=F32) * scale
        )
        grad_queries = (
            rotate(grad_q.reshape(stretch, heads_q, HDIM), position, -1.0)
            .astype(BF16)
            .reshape(stretch, heads_q * HDIM)
        )
        grad_keys = (
            rotate(grad_kv_local[:, :kv_width].reshape(stretch, heads_kv, HDIM), position, -1.0)
            .astype(BF16)
            .reshape(stretch, kv_width)
        )
        grad_values = grad_kv_local[:, kv_width:].astype(BF16)
        grad_qkv = jnp.concatenate([grad_queries, grad_keys, grad_values], axis=1)
        grad_wqkv = reduce_weight(
            tdot(normed1, grad_qkv).astype(BF16), ("A1", "B1", "A2"), axes, place
        )
        q_width = heads_q * HDIM
        grad_wquery = grad_wqkv[:, :q_width]
        grad_wkey = grad_wqkv[:, q_width : q_width + kv_width]
        grad_wvalue = grad_wqkv[:, q_width + kv_width :]
        grad_normed1 = tensor_sum(
            (
                rdot(grad_queries, w_query) + rdot(grad_keys, w_key) + rdot(grad_values, w_value)
            ).astype(BF16),
            n_tensor,
        )
        scaled_one = grad_normed1 * norm1_gain
        grad_gain_one = jnp.sum(grad_normed1 * inputs * inv_one, axis=0)
        grad_in = (
            grad_hidden
            + inv_one * scaled_one
            - inputs
            * (inv_one * inv_one * inv_one)
            * jnp.mean(scaled_one * inputs, axis=1, keepdims=True)
        ).astype(BF16)
        gains = jnp.stack([grad_gain_one, grad_gain_two]).astype(BF16)
        for axis in axes:
            gains = add(gains, axis.swap(gains))
        gains = gains.astype(F32)
        return (
            block_output,
            grad_in.reshape(1, stretch, width),
            gains[0],
            grad_wquery,
            grad_wkey,
            grad_wvalue,
            grad_wout,
            gains[1],
            grad_wgate,
            grad_wup,
            grad_wdown,
        )

    return shards


def solution(mesh):
    shape = dict(mesh.shape)
    rows, columns = P("tensor", None), P(None, "tensor")
    tokens = P("dp", "ctx", None)
    return jax.shard_map(
        make_shards(shape["dp"], shape["ctx"], shape["tensor"]),
        mesh=mesh,
        in_specs=(
            tokens,
            P("dp", None),
            P("dp", "ctx"),
            tokens,
            P(),
            columns,
            columns,
            columns,
            rows,
            P(),
            columns,
            columns,
            rows,
        ),
        out_specs=(
            tokens,
            tokens,
            P(),
            columns,
            columns,
            columns,
            rows,
            P(),
            columns,
            columns,
            rows,
        ),
        check_vma=False,
    )
```
